256 devices in a mesh: layer: 4 (over z_lo, core), feat: 64 (over y, z_hi, x).
Axes of the slice: x: 4, y: 4, z: 8 (z_hi: 4, z_lo: 2; z = z_hi * 2 + z_lo), core: 2. Of those that a mesh axis runs over, the one named last changes fastest.
Arguments:
- activations: bfloat16 [512, 4, 2304], P('feat', 'layer'), may hold values from -6 to 6
- enc_weight: bfloat16 [4, 2304, 65536], P('layer', None, 'feat'), may hold values from -0.0625 to 0.0625
- dec_weight: bfloat16 [4, 65536, 2304], P('layer', 'feat'), may hold values from -0.03125 to 0.03125
- enc_bias: float32 [65536], P('feat'), may hold values from -3 to 3
- threshold: float32 [65536], P('feat'), may hold values from 0.1 to 1
- dec_bias: float32 [4, 2304], P('layer'), may hold values from -3 to 3
- token_mask: int32 [512], replicated, may hold values 0 or 1
Outputs:
- squared_error: float32 [512, 4], P('feat', 'layer')
- latent_grad: float32 [512, 65536], P(None, 'feat')
- input_grad: bfloat16 [512, 4, 2304], P('feat', 'layer')
The draws below stay inside these ranges and needn't reach their ends.
All inputs are finite; a program needn't handle non-finite values.
Results may differ from the reference program's by a relative error of at most 0.015.
Values may be sent and summed in bfloat16 or wider, within the bound.
A program may use at most 64 MiB of HBM per device.

```python
import math
import jax
import jax.numpy as jnp

D = 2304
LAYERS = 4
FEATURES = 65536
TOKENS = 512


def set_ends(result, rng, smallest, largest):
    spot = [jax.random.randint(jax.random.fold_in(rng, axis), (), 0, length) for axis, length in enumerate(result.shape)]
    longest = result.shape.index(max(result.shape))
    next_to = spot[:longest] + [(spot[longest] + 1) % result.shape[longest]] + spot[longest + 1:]
    return result.at[tuple(spot)].set(smallest).at[tuple(next_to)].set(largest)


def shard_levels(key, shape, shards, smallest, largest):
    def one(axis_at, blocks):
        draws = jax.random.uniform(jax.random.fold_in(jax.random.fold_in(key, 6), axis_at), (blocks,), jnp.float32, smallest / len(shards), largest / len(shards))
        return jnp.repeat(jnp.exp(draws), shape[axis_at] // blocks).reshape((-1,) + (1,) * (len(shape) - axis_at - 1))

    gain = one(*shards[0])
    for cut in shards[1:]:
        gain = gain * one(*cut)
    return gain


def scatter_about(key, extent, deviation, bound, split=(), held_as=jnp.bfloat16):
    factor_of = shard_levels(key, extent, split, -0.22, 0.18) if split else 1.0
    result = jax.random.normal(key, extent, jnp.float32) * deviation * factor_of
    return jnp.minimum(jnp.maximum(result, -bound), bound).astype(held_as)


def setup_inputs(seed: int = 0) -> dict:
    key_of = jax.random.split(jax.random.key(seed), 8)
    return {
        "activations": scatter_about(key_of[0], (TOKENS, LAYERS, D), 1.0, 6.0, ((0, 64), (1, 4))),
        "enc_weight": scatter_about(key_of[1], (LAYERS, D, FEATURES), (LAYERS * D) ** -0.5, 0.0625, ((0, 4), (2, 64))),
        "dec_weight": scatter_about(key_of[2], (LAYERS, FEATURES, D), (FEATURES // 2) ** -0.5, 0.03125, ((0, 4), (1, 64))),
        "enc_bias": scatter_about(key_of[3], (FEATURES,), 0.5, 3.0, ((0, 64),), jnp.float32),
        "threshold": jnp.clip(jnp.exp(math.log(1.0) - 2.3025851 * jax.random.uniform(key_of[4], (FEATURES,), jnp.float32) ** shard_levels(key_of[4], (FEATURES,), ((0, 64),), -0.2, 0.2)), 0.1, 1.0),
        "dec_bias": scatter_about(key_of[5], (LAYERS, D), 0.5, 3.0, ((0, 4),), jnp.float32),
        "token_mask": set_ends((jax.random.randint(key_of[6], (TOKENS,), 0, 4) < 3).astype(jnp.int32), jax.random.fold_in(key_of[6], 1), 0, 1),
    }


jump_scale = 0.25


def reference(activations, enc_weight, dec_weight, enc_bias, threshold, dec_bias, token_mask):
    acts_wide = activations.astype(jnp.float32)
    enc_wide = enc_weight.astype(jnp.float32)
    dec_wide = dec_weight.astype(jnp.float32)
    preact = jnp.einsum('tld,ldf->tf', acts_wide, enc_wide) + enc_bias
    gating = jax.nn.sigmoid((preact - threshold) / jump_scale)
    latent = (preact * gating).astype(jnp.bfloat16)
    gate_slope = gating + preact * gating * (1.0 - gating) / jump_scale
    rebuilt = jnp.einsum('tf,lfd->tld', latent.astype(jnp.float32), dec_wide)
    weights_mask = token_mask.astype(jnp.float32)[:, None, None]
    error = weights_mask * (rebuilt + dec_bias[None, :, :] - acts_wide)
    squared_error = jnp.mean(error * error, axis=-1)
    error_half = error.astype(jnp.bfloat16)
    latent_grad = jnp.einsum('tld,lfd->tf', error_half.astype(jnp.float32), dec_wide)
    preact_grad = (latent_grad * gate_slope).astype(jnp.bfloat16)
    grad_terms = jnp.einsum('tf,ldf->tld', preact_grad.astype(jnp.float32), enc_wide)
    input_grad = (grad_terms - error).astype(jnp.bfloat16)
    return squared_error, latent_grad, input_grad
```

```python
import functools

import jax
import jax.numpy as jnp
from jax import lax
from jax.experimental import pallas as pl
from jax.experimental.pallas import tpu as pltpu
from jax.sharding import Mesh
from jax.sharding import PartitionSpec as P

FEAT = ("y", "zh", "x")
LAYER = ("zl", "co")
MESH = pl.DeviceIdType.MESH
BF = jnp.bfloat16
F32 = jnp.float32
JUMP = 0.25

N = 4
C = 2
S = N // C
ROWS = 8
R = S * ROWS
M = N * N * R
HM = M // 2
LAG = 3


def kernel(
    acts, enc_hbm, dec_hbm, enc_bias, threshold, dec_bias, mask,
    sq_out, ig_out, lg_out,
    enc, dec, ag, zbuf, ps, f1, a1, b1, ps2, f2, a2, b2, ps3, zr,
    keep, dsend, drecv, zs, zv, full, lat, slope, err, errh,
    wsem, osem, zsnd, zrcv, agsnd, agrcv, rssnd, rsrcv, zrsnd, zrrcv, lsnd, lrcv,
):
    depth = ag.shape[-1]
    feats = lat.shape[-1]
    half = depth // 2
    cut = (half // 256 + 1) * 128
    x, y, zh = lax.axis_index("x"), lax.axis_index("y"), lax.axis_index("zh")
    zl, co = lax.axis_index("zl"), lax.axis_index("co")
    at = {"x": x, "y": y, "zh": zh}

    def step(axis, by):
        return lax.rem(at[axis] + (by + N) % N, N)

    def to(axis, by):
        return {axis: step(axis, by)}

    enc_copy = pltpu.make_async_copy(enc_hbm, enc, wsem.at[0])
    dec_copy = pltpu.make_async_copy(dec_hbm, dec, wsem.at[1])
    enc_copy.start()
    dec_copy.start()

    barrier = pltpu.get_barrier_semaphore()
    peers = [to("x", 1), to("x", -1), to("y", 1), to("y", -1)]
    peers += [to("zh", 1), to("zh", 2), to("zh", 3), {"zl": 1 - zl}, {"co": 1 - co}]
    for peer in peers:
        pl.semaphore_signal(barrier, inc=1, device_id=peer, device_id_type=MESH)
    pl.semaphore_wait(barrier, len(peers))

    def remote(src, dst, send, recv, peer):
        return pltpu.make_async_remote_copy(
            src_ref=src, dst_ref=dst, send_sem=send, recv_sem=recv,
            device_id=peer, device_id_type=MESH,
        )

    def cols(h, part):
        base, length = {None: (0, half), 0: (0, cut), 1: (cut, half - cut)}[part]
        return pl.ds(h * half + base, length)

    class Gather:
        def __init__(self, axis, block, send, recv):
            self.axis, self.block, self.send, self.recv = axis, block, send, recv
            self.copies = []

        def push(self, pos, part, by):
            n = len(self.copies)
            ref = self.block(pos, part)
            copy = remote(ref, ref, self.send.at[n], self.recv.at[n], to(self.axis, by))
            copy.start()
            self.copies.append(copy)

        def start(self):
            self.push(at[self.axis], None, 1)
            self.push(at[self.axis], None, -1)

        def middle(self):
            self.copies[0].wait_recv()
            self.push(step(self.axis, -1), 0, 1)
            self.copies[1].wait_recv()
            self.push(step(self.axis, 1), 1, -1)

        def finish(self):
            self.copies[2].wait_recv()
            self.copies[3].wait_recv()
            for copy in self.copies:
                copy.wait_send()

    class Scatter:
        def __init__(self, axis, block, f, a, b, send, recv):
            self.axis, self.block, self.f, self.a, self.b = axis, block, f, a, b
            self.send, self.recv, self.copies = send, recv, []

        def push(self, src, dst, by):
            n = len(self.copies)
            copy = remote(src, dst, self.send.at[n], self.recv.at[n], to(self.axis, by))
            copy.start()
            self.copies.append(copy)

        def slot(self, buf, part):
            return buf.at[(slice(None),) * (len(buf.shape) - 1) + (cols(0, part),)]

        def start(self):
            far = step(self.axis, 2)
            self.push(self.block(far, 0), self.slot(self.f, 0), 1)
            self.push(self.block(far, 1), self.slot(self.f, 1), -1)
            self.push(self.block(step(self.axis, 1), 1), self.slot(self.a, 1), 1)
            self.push(self.block(step(self.axis, -1), 0), self.slot(self.b, 0), -1)

        def middle(self):
            for part, by, into in ((0, 1, self.a), (1, -1, self.b)):
                self.copies[part].wait_recv()
                here = self.slot(self.f, part)
                own = self.block(step(self.axis, by), part)
                here[...] = (here[...].astype(F32) + own[...].astype(F32)).astype(BF)
                self.push(here, self.slot(into, part), by)

        def finish(self):
            for copy in self.copies[2:]:
                copy.wait_recv()
            total = self.block(at[self.axis], None)[...].astype(F32)
            total = total + self.a[...].astype(F32) + self.b[...].astype(F32)
            for copy in self.copies:
                copy.wait_send()
            return total

    def chunk(c):
        def z_send(src):
            for s in range(S):
                @pl.when(zh == c * S + s)
                def _():
                    zbuf[c, s] = src[...]
                    for k in (1, 2, 3):
                        remote(src, zbuf.at[c, s], zsnd.at[k - 1], zrcv.at[c, s], to("zh", k)).start()

        def z_wait(src):
            for s in range(S):
                one = remote(src, zbuf.at[c, s], zsnd.at[0], zrcv.at[c, s], to("zh", 1))

                @pl.when(zh != c * S + s)
                def _():
                    one.wait_recv()

                @pl.when(zh == c * S + s)
                def _():
                    for k in (1, 2, 3):
                        remote(src, zbuf.at[c, s], zsnd.at[k - 1], zrcv.at[c, s], to("zh", k)).wait_send()

            ag[c, y, x] = zbuf[c].astype(F32).reshape(R, depth).astype(BF)

        def gather_stages(src):
            near = [
                Gather("x", lambda i, p: ag.at[c, y, i, :, cols(0, p)], agsnd.at[c, 0, 0], agrcv.at[c, 0, 0]),
                Gather("y", lambda i, p: ag.at[c, i, x, :, cols(1, p)], agsnd.at[c, 1, 0], agrcv.at[c, 1, 0]),
            ]
            wide = [
                Gather("y", lambda i, p: ag.at[c, i, :, :, cols(0, p)], agsnd.at[c, 0, 1], agrcv.at[c, 0, 1]),
                Gather("x", lambda i, p: ag.at[c, :, i, :, cols(1, p)], agsnd.at[c, 1, 1], agrcv.at[c, 1, 1]),
            ]

            def begin():
                z_wait(src)
                for g in near:
                    g.start()

            def forward():
                for g in near:
                    g.middle()

            def widen():
                for g, w in zip(near, wide):
                    g.finish()
                    w.start()

            def forward_wide():
                for w in wide:
                    w.middle()

            def end():
                for w in wide:
                    w.finish()

            return [begin, forward, widen, forward_wide, end]

        def layer_stages(lhs, rhs, tile):
            copies = {}

            def multiply():
                def one(j, carry):
                    where = pl.ds(pl.multiple_of(j * tile, tile), tile)
                    value = rhs(lhs, where)
                    low, high = value[:HM], value[HM:]
                    keep[c, :, where] = jnp.where(co == 0, low, high)
                    dsend[c, :, where] = jnp.where(co == 0, high, low).astype(BF)
                    return carry

                lax.fori_loop(0, feats // tile, one, 0)
                copies[0] = remote(dsend.at[c], drecv.at[c], lsnd.at[c, 0], lrcv.at[c, 0], {"co": 1 - co})
                copies[0].start()

            def pair():
                copies[0].wait()
                zs[c] = (keep[c] + drecv[c].astype(F32)).astype(BF)
                copies[1] = remote(zs.at[c], zv.at[c], lsnd.at[c, 1], lrcv.at[c, 1], {"zl": 1 - zl})
                copies[1].start()

            def share():
                copies[1].wait()
                full[c, co] = (zs[c].astype(F32) + zv[c].astype(F32)).astype(BF)
                ref = full.at[c, co]
                copies[2] = remote(ref, ref, lsnd.at[c, 2], lrcv.at[c, 2], {"co": 1 - co})
                copies[2].start()

            def end():
                copies[2].wait()

            return [multiply, pair, share, end]

        def scatter_stages(multiply):
            wide = [
                Scatter("y", lambda i, p: ps.at[c, i, :, :, cols(0, p)], f1.at[c, 0], a1.at[c, 0], b1.at[c, 0],
                        rssnd.at[c, 0, 0], rsrcv.at[c, 0, 0]),
                Scatter("x", lambda i, p: ps.at[c, :, i, :, cols(1, p)], f1.at[c, 1], a1.at[c, 1], b1.at[c, 1],
                        rssnd.at[c, 1, 0], rsrcv.at[c, 1, 0]),
            ]
            near = [
                Scatter(axis, lambda i, p, h=h: ps2.at[c, h, i, :, cols(0, p)], f2.at[c, h], a2.at[c, h], b2.at[c, h],
                        rssnd.at[c, h, 1], rsrcv.at[c, h, 1])
                for h, axis in enumerate(("x", "y"))
            ]

            def begin():
                for h in range(2):
                    multiply(h)
                    wide[h].start()

            def forward():
                for w in wide:
                    w.middle()

            def narrow():
                for h in range(2):
                    ps2[c, h] = wide[h].finish().astype(BF)
                    near[h].start()

            def forward_near():
                for g in near:
                    g.middle()

            def z_out():
                for h in range(2):
                    ps3[c, :, :, cols(h, None)] = near[h].finish().reshape(S, ROWS, half).astype(BF)
                for s in range(S):
                    @pl.when(zh != c * S + s)
                    def _():
                        k = lax.rem(zh - (c * S + s) + N, N) - 1
                        remote(ps3.at[c, s], zr.at[k], zrsnd.at[c, s], zrrcv.at[k], {"zh": c * S + s}).start()

            return [begin, forward, narrow, forward_near, z_out]

        def owned(then):
            for s in range(S):
                @pl.when(zh != c * S + s)
                def _():
                    remote(ps3.at[c, s], zr.at[0], zrsnd.at[c, s], zrrcv.at[0], {"zh": c * S + s}).wait_send()

                @pl.when(zh == c * S + s)
                def _():
                    total = ps3[c, s].astype(F32)
                    for k in range(3):
                        remote(ps3.at[c, s], zr.at[k], zrsnd.at[c, s], zrrcv.at[k], to("zh", 1)).wait_recv()
                        total = total + zr[k].astype(F32)
                    then(total)

        def z_first():
            z_send(acts)

        def to_latent():
            for r in range(2):
                preact = full[c, r].astype(F32) + enc_bias[...]
                gating = jax.nn.sigmoid((preact - threshold[...]) * (1.0 / JUMP))
                value = preact * gating
                lat[c, pl.ds(r * HM, HM)] = value.astype(BF)
                slope[c, pl.ds(r * HM, HM)] = gating + value * (1.0 - gating) * (1.0 / JUMP)

        def to_preact_grad():
            pltpu.make_async_copy(full.at[c], lg_out.at[c], osem.at[c]).start()
            for r in range(2):
                rows = pl.ds(r * HM, HM)
                lat[c, rows] = (full[c, r].astype(F32) * slope[c, rows]).astype(BF)

        def to_error():
            def then(total):
                row = lax.broadcasted_iota(jnp.int32, (ROWS, 1), 0)
                first = ((y * N + zh) * N + x) * ROWS
                keeps = jnp.zeros((ROWS, 1), jnp.int32)
                for i in range(ROWS):
                    keeps = jnp.where(row == i, mask[first + i], keeps)
                value = keeps.astype(F32) * (total + dec_bias[...] - acts[...].astype(F32))
                err[...] = value
                errh[...] = value.astype(BF)
                sq_out[...] = jnp.sum(value * value, axis=1, keepdims=True) * (1.0 / depth)

            owned(then)
            z_send(errh)

        def to_input_grad():
            def then(total):
                ig_out[...] = (total - err[...]).astype(BF)

            owned(then)

        def dot(a, b, dims):
            return lax.dot_general(a, b, (dims, ((), ())), preferred_element_type=F32)

        def tokens():
            return ag[c].reshape(M, depth)

        def encode(lhs, where):
            return dot(lhs(), enc[:, where], ((1,), (0,)))

        def decode_back(lhs, where):
            return dot(lhs(), dec[where, :], ((1,), (1,)))

        def tiles(h):
            begin = 0
            while begin < half:
                length = min(512, half - begin)
                yield pl.ds(h * half + begin, length), length
                begin += length

        def decode(h):
            for where, length in tiles(h):
                value = dot(lat[c], dec[:, where], ((1,), (0,)))
                ps[c, :, :, :, where] = value.reshape(N, N, R, length).astype(BF)

        def encode_back(h):
            for where, length in tiles(h):
                value = dot(lat[c], enc[where, :], ((1,), (1,)))
                ps[c, :, :, :, where] = value.reshape(N, N, R, length).astype(BF)

        def wait_enc():
            if c == 0:
                enc_copy.wait()

        def wait_dec():
            if c == 0:
                dec_copy.wait()

        def joined(*parts):
            def run():
                for part in parts:
                    part()

            return run

        g1, l1, s1 = gather_stages(acts), layer_stages(tokens, encode, 256), scatter_stages(decode)
        g2, l2, s2 = gather_stages(errh), layer_stages(tokens, decode_back, 256), scatter_stages(encode_back)
        return [
            z_first,
            *g1[:-1],
            joined(g1[-1], wait_enc, l1[0]),
            *l1[1:-1],
            joined(l1[-1], to_latent, wait_dec, s1[0]),
            *s1[1:],
            to_error,
            *g2[:-1],
            joined(g2[-1], l2[0]),
            *l2[1:-1],
            joined(l2[-1], to_preact_grad, s2[0]),
            *s2[1:],
            to_input_grad,
        ]

    plans = [chunk(c) for c in range(C)]
    length = len(plans[0])
    for tick in range(length + LAG * (C - 1)):
        for c in range(C):
            if 0 <= tick - LAG * c < length:
                plans[c][tick - LAG * c]()
    for c in range(C):
        pltpu.make_async_copy(full.at[c], lg_out.at[c], osem.at[c]).wait()


def shards(activations, enc_weight, dec_weight, enc_bias, threshold, dec_bias, token_mask):
    depth, feats = enc_weight.shape[1:]
    half = depth // 2
    vmem, any_space = pl.BlockSpec(memory_space=pltpu.VMEM), pl.BlockSpec(memory_space=pl.ANY)
    dma = pltpu.SemaphoreType.DMA
    scratch = [
        pltpu.VMEM((depth, feats), BF),
        pltpu.VMEM((feats, depth), BF),
        pltpu.VMEM((C, N, N, R, depth), BF),
        pltpu.VMEM((C, S, ROWS, depth), BF),
        pltpu.VMEM((C, N, N, R, depth), BF),
        *[pltpu.VMEM((C, 2, N, R, half), BF)] * 3,
        pltpu.VMEM((C, 2, N, R, half), BF),
        *[pltpu.VMEM((C, 2, R, half), BF)] * 3,
        pltpu.VMEM((C, S, ROWS, depth), BF),
        pltpu.VMEM((N - 1, ROWS, depth), BF),
        pltpu.VMEM((C, HM, feats), F32),
        *[pltpu.VMEM((C, HM, feats), BF)] * 4,
        pltpu.VMEM((C, 2, HM, feats), BF),
        pltpu.VMEM((C, M, feats), BF),
        pltpu.VMEM((C, M, feats), F32),
        pltpu.VMEM((ROWS, depth), F32),
        pltpu.VMEM((ROWS, depth), BF),
        dma((2,)),
        dma((C,)),
        dma((3,)), dma((C, S)),
        dma((C, 2, 2, 4)), dma((C, 2, 2, 4)),
        dma((C, 2, 2, 6)), dma((C, 2, 2, 6)),
        dma((C, S)), dma((3,)),
        dma((C, 3)), dma((C, 3)),
    ]
    sq, ig, lg = pl.pallas_call(
        kernel,
        out_shape=(
            jax.ShapeDtypeStruct((ROWS, 1), F32),
            jax.ShapeDtypeStruct((ROWS, depth), BF),
            jax.ShapeDtypeStruct((C, 2, HM, feats), BF),
        ),
        in_specs=[vmem, any_space, any_space, vmem, vmem, vmem, pl.BlockSpec(memory_space=pltpu.SMEM)],
        out_specs=(vmem, vmem, any_space),
        scratch_shapes=scratch,
        compiler_params=pltpu.CompilerParams(
            collective_id=0, has_side_effects=True, vmem_limit_bytes=48 * 1024 * 1024
        ),
    )(
        activations[:, 0], enc_weight[0], dec_weight[0], enc_bias[None], threshold[None], dec_bias, token_mask,
    )
    lg = lg.reshape(C, N, N, S, ROWS, feats).transpose(1, 0, 3, 2, 4, 5)
    return sq, lg.reshape(N * N * N * ROWS, feats).astype(F32), ig[:, None]


def solution(mesh):
    finer = Mesh(mesh.devices.reshape(2, 2, N, N, N), LAYER + FEAT)
    return jax.shard_map(
        shards,
        mesh=finer,
        in_specs=(
            P(FEAT, LAYER, None),
            P(LAYER, None, FEAT),
            P(LAYER, FEAT, None),
            P(FEAT),
            P(FEAT),
            P(LAYER, None),
            P(),
        ),
        out_specs=(P(FEAT, LAYER), P(None, FEAT), P(FEAT, LAYER, None)),
        check_vma=False,
    )
```

```python
import functools

import jax
import jax.numpy as jnp
from jax import lax
from jax.experimental import pallas as pl
from jax.experimental.pallas import tpu as pltpu
from jax.sharding import Mesh
from jax.sharding import PartitionSpec as P

FEAT = ("y", "zh", "x")
LAYER = ("zl", "co")
MESH = pl.DeviceIdType.MESH
BF = jnp.bfloat16
F32 = jnp.float32
JUMP = 0.25

N = 4
C = 4
S = N // C
ROWS = 8
R = S * ROWS
M = N * N * R
HM = M // 2
PIECES = 2
TURNS = (
    0, 2, 1, 3, 0, 2, 1, 3, 0, 1, 0, 2, 1, 3, 0, 2, 0, 0, 1, 0, 3, 1, 1, 1, 2, 0, 2, 0, 2,
    3, 2, 0, 3, 1, 1, 3, 1, 0, 2, 3, 2, 2, 3, 1, 0, 2, 1, 3, 0, 2, 3, 1, 2, 0, 3, 1, 3, 2,
    0, 1, 3, 0, 2, 1, 0, 3, 1, 2, 0, 3, 0, 0, 2, 1, 0, 1, 3, 1, 2, 0, 1, 2, 3, 2, 0, 2, 1,
    0, 1, 3, 3, 3, 2, 2, 0, 3, 1, 2, 3, 3, 0, 3, 2, 0, 1, 3, 2, 1, 3, 2, 1, 3, 2, 1, 0, 3,
)


def kernel(
    acts_hbm, enc_hbm, dec_hbm, enc_bias_hbm, threshold_hbm, dec_bias_hbm, mask_hbm,
    sq_out, ig_out, lg_out,
    acts, enc_bias, threshold, dec_bias, mask, enc, dec, ag, zbuf, ps, f1, a1, b1, ps2, f2, a2, b2, ps3, zr,
    keep, dsend, drecv, zs, zv, full, lat, slope, err, errh, sq, ig,
    wsem, osem, zsnd, zrcv, agsnd, agrcv, rssnd, rsrcv, zrsnd, zrrcv, lsnd, lrcv,
):
    depth = ag.shape[-1]
    feats = lat.shape[-1]
    half = depth // 2
    cut = (half // 256 + 1) * 128
    x, y, zh = lax.axis_index("x"), lax.axis_index("y"), lax.axis_index("zh")
    zl, co = lax.axis_index("zl"), lax.axis_index("co")
    at = {"x": x, "y": y, "zh": zh}

    def step(axis, by):
        return lax.rem(at[axis] + (by + N) % N, N)

    def to(axis, by):
        return {axis: step(axis, by)}

    acts_copy, enc_copy, dec_copy, *small = [
        pltpu.make_async_copy(src, dst, wsem.at[n])
        for n, (src, dst) in enumerate((
            (acts_hbm, acts), (enc_hbm, enc), (dec_hbm, dec), (enc_bias_hbm, enc_bias),
            (threshold_hbm, threshold), (dec_bias_hbm, dec_bias), (mask_hbm, mask),
        ))
    ]
    for copy in (acts_copy, *small, enc_copy, dec_copy):
        copy.start()

    barrier = pltpu.get_barrier_semaphore()
    peers = [to(axis, by) for axis in ("x", "y", "zh") for by in (1, 2, 3)]
    peers += [{"zl": 1 - zl}, {"co": 1 - co}]
    for peer in peers:
        pl.semaphore_signal(barrier, inc=1, device_id=peer, device_id_type=MESH)
    pl.semaphore_wait(barrier, len(peers))
    acts_copy.wait()

    def remote(src, dst, send, recv, peer):
        return pltpu.make_async_remote_copy(
            src_ref=src, dst_ref=dst, send_sem=send, recv_sem=recv,
            device_id=peer, device_id_type=MESH,
        )

    def cols(h, part):
        base, length = {None: (0, half), 0: (0, cut), 1: (cut, half - cut)}[part]
        return pl.ds(h * half + base, length)

    class Ring:
        def __init__(self, axis, block, send, recv):
            self.axis, self.block, self.send, self.recv = axis, block, send, recv
            self.copies = []

        def push(self, src, dst, by):
            n = len(self.copies)
            copy = remote(src, dst, self.send.at[n], self.recv.at[n], to(self.axis, by))
            copy.start()
            self.copies.append(copy)

        def arrived(self, *which):
            for n in which:
                self.copies[n].wait_recv()

        def sent(self):
            for copy in self.copies:
                copy.wait_send()

    class Gather(Ring):
        def pass_on(self, pos, part, by):
            ref = self.block(pos, part)
            self.push(ref, ref, by)

        def start(self):
            me = at[self.axis]
            self.pass_on(me, 0, 1)
            self.pass_on(me, 1, -1)
            self.pass_on(me, 1, 1)
            self.pass_on(me, 0, -1)

        def middle(self):
            self.arrived(0)
            self.pass_on(step(self.axis, -1), 0, 1)
            self.arrived(1)
            self.pass_on(step(self.axis, 1), 1, -1)

        def finish(self):
            self.arrived(2, 3, 4, 5)
            self.sent()

    class DirectGather(Ring):
        def start(self):
            ref = self.block(at[self.axis], None)
            for by in (2, 1, -1):
                self.push(ref, ref, by)

        def finish(self):
            self.arrived(0, 1, 2)
            self.sent()

    class Scatter(Ring):
        def __init__(self, axis, block, f, a, b, send, recv):
            super().__init__(axis, block, send, recv)
            self.f, self.a, self.b = f, a, b

        def slot(self, buf, part):
            return buf.at[(slice(None),) * (len(buf.shape) - 1) + (cols(0, part),)]

        def start(self):
            far = step(self.axis, 2)
            self.push(self.block(far, 0), self.slot(self.f, 0), 1)
            self.push(self.block(far, 1), self.slot(self.f, 1), -1)
            self.push(self.block(step(self.axis, 1), 1), self.slot(self.a, 1), 1)
            self.push(self.block(step(self.axis, -1), 0), self.slot(self.b, 0), -1)

        def middle(self):
            for part, by, into in ((0, 1, self.a), (1, -1, self.b)):
                self.arrived(part)
                here = self.slot(self.f, part)
                own = self.block(step(self.axis, by), part)
                here[...] = (here[...].astype(F32) + own[...].astype(F32)).astype(BF)
                self.push(here, self.slot(into, part), by)

        def finish(self):
            self.arrived(2, 3, 4, 5)
            total = self.block(at[self.axis], None)[...].astype(F32)
            total = total + self.a[...].astype(F32) + self.b[...].astype(F32)
            self.sent()
            return total

    class DirectScatter(Scatter):
        def start(self):
            for by, into in ((2, self.f), (1, self.a), (-1, self.b)):
                self.push(self.block(step(self.axis, by), None), into, by)

        def finish(self):
            self.arrived(0, 1, 2)
            total = self.block(at[self.axis], None)[...].astype(F32) + self.f[...].astype(F32)
            total = total + self.a[...].astype(F32) + self.b[...].astype(F32)
            self.sent()
            return total

    def grads_out(c):
        for j in range(M // ROWS):
            row = ((j // (N * S) * N + c * S + j % S) * N + j // S % N) * ROWS
            yield pltpu.make_async_copy(full.at[c, pl.ds(j * ROWS, ROWS)], lg_out.at[pl.ds(row, ROWS)], osem.at[c])

    def wait_outs(c):
        pltpu.make_async_copy(full.at[c], lg_out.at[pl.ds(0, M)], osem.at[c]).wait()

        @pl.when(zh // S == c)
        def _():
            pltpu.make_async_copy(sq, sq_out, osem.at[C]).wait()

    def chunk(c):
        def z_send(src):
            for s in range(S):
                @pl.when(zh == c * S + s)
                def _():
                    zbuf[c, s] = src[...]
                    for k in (1, 2, 3):
                        remote(src, zbuf.at[c, s], zsnd.at[k - 1], zrcv.at[c, s], to("zh", k)).start()

        def z_wait(src):
            for s in range(S):
                one = remote(src, zbuf.at[c, s], zsnd.at[0], zrcv.at[c, s], to("zh", 1))

                @pl.when(zh != c * S + s)
                def _():
                    one.wait_recv()

                @pl.when(zh == c * S + s)
                def _():
                    for k in (1, 2, 3):
                        remote(src, zbuf.at[c, s], zsnd.at[k - 1], zrcv.at[c, s], to("zh", k)).wait_send()

            ag[c, y, x] = zbuf[c].astype(F32).reshape(R, depth).astype(BF)

        def gather_stages(src):
            near = [
                DirectGather("x", lambda i, p: ag.at[c, y, i, :, cols(0, p)], agsnd.at[c, 0, 0], agrcv.at[c, 0, 0]),
                DirectGather("y", lambda i, p: ag.at[c, i, x, :, cols(1, p)], agsnd.at[c, 1, 0], agrcv.at[c, 1, 0]),
            ]
            wide = [
                Gather("y", lambda i, p: ag.at[c, i, :, :, cols(0, p)], agsnd.at[c, 0, 1], agrcv.at[c, 0, 1]),
                Gather("x", lambda i, p: ag.at[c, :, i, :, cols(1, p)], agsnd.at[c, 1, 1], agrcv.at[c, 1, 1]),
            ]

            def begin():
                z_wait(src)
                for g in near:
                    g.start()

            def widen():
                for g, w in zip(near, wide):
                    g.finish()
                    w.start()

            def forward():
                for w in wide:
                    w.middle()

            def end():
                for w in wide:
                    w.finish()

            return [begin, widen, forward, end]

        def layer_stages(lhs, rhs, tile):
            copies = {}
            width = feats // PIECES

            def exchange(kind, p, src, dst, peer):
                copies[kind, p] = remote(src, dst, lsnd.at[c, kind, p], lrcv.at[c, kind, p], peer)
                copies[kind, p].start()

            def multiply(p):
                def one(j, carry):
                    where = pl.ds(pl.multiple_of(p * width + j * tile, tile), tile)
                    value = rhs(lhs, where)
                    low, high = value[:HM], value[HM:]
                    keep[c, :, where] = jnp.where(co == 0, low, high)
                    dsend[c, :, where] = jnp.where(co == 0, high, low).astype(BF)
                    return carry

                lax.fori_loop(0, width // tile, one, 0)
                piece = pl.ds(p * width, width)
                exchange(0, p, dsend.at[c, :, piece], drecv.at[c, :, piece], {"co": 1 - co})

            def pair(p):
                copies[0, p].wait()
                piece = pl.ds(p * width, width)
                zs[c, :, piece] = (keep[c, :, piece] + drecv[c, :, piece].astype(F32)).astype(BF)
                exchange(1, p, zs.at[c, :, piece], zv.at[c, :, piece], {"zl": 1 - zl})

            def share(p):
                copies[1, p].wait()
                piece = pl.ds(p * width, width)
                mine = pl.ds(pl.multiple_of(co * HM, HM), HM)
                full[c, mine, piece] = (zs[c, :, piece].astype(F32) + zv[c, :, piece].astype(F32)).astype(BF)
                ref = full.at[c, mine, piece]
                exchange(2, p, ref, ref, {"co": 1 - co})

            def end():
                for p in range(PIECES):
                    copies[2, p].wait()

            pieces = range(PIECES)
            return [
                *[functools.partial(multiply, p) for p in pieces],
                *[functools.partial(pair, p) for p in pieces],
                *[functools.partial(share, p) for p in pieces],
                end,
            ]

        def scatter_stages(multiply):
            wide = [
                Scatter("y", lambda i, p: ps.at[c, i, :, :, cols(0, p)], f1.at[c, 0], a1.at[c, 0], b1.at[c, 0],
                        rssnd.at[c, 0, 0], rsrcv.at[c, 0, 0]),
                Scatter("x", lambda i, p: ps.at[c, :, i, :, cols(1, p)], f1.at[c, 1], a1.at[c, 1], b1.at[c, 1],
                        rssnd.at[c, 1, 0], rsrcv.at[c, 1, 0]),
            ]
            near = [
                DirectScatter(axis, lambda i, p, h=h: ps2.at[c, h, i, :, cols(0, p)], f2.at[c, h], a2.at[c, h], b2.at[c, h],
                        rssnd.at[c, h, 1], rsrcv.at[c, h, 1])
                for h, axis in enumerate(("x", "y"))
            ]

            def begin():
                for h in range(2):
                    multiply(h)
                    wide[h].start()

            def forward():
                for w in wide:
                    w.middle()

            def narrow():
                for h in range(2):
                    ps2[c, h] = wide[h].finish().astype(BF)
                    near[h].start()

            def z_out():
                for h in range(2):
                    ps3[c, :, :, cols(h, None)] = near[h].finish().reshape(S, ROWS, half).astype(BF)
                for s in range(S):
                    @pl.when(zh != c * S + s)
                    def _():
                        k = lax.rem(zh - (c * S + s) + N, N) - 1
                        remote(ps3.at[c, s], zr.at[k], zrsnd.at[c, s], zrrcv.at[k], {"zh": c * S + s}).start()

            return [begin, forward, narrow, z_out]

        def owned(then):
            for s in range(S):
                @pl.when(zh != c * S + s)
                def _():
                    remote(ps3.at[c, s], zr.at[0], zrsnd.at[c, s], zrrcv.at[0], {"zh": c * S + s}).wait_send()

                @pl.when(zh == c * S + s)
                def _():
                    total = ps3[c, s].astype(F32)
                    for k in range(3):
                        remote(ps3.at[c, s], zr.at[k], zrsnd.at[c, s], zrrcv.at[k], to("zh", 1)).wait_recv()
                        total = total + zr[k].astype(F32)
                    then(total)

        def z_first():
            z_send(acts)

        def to_latent():
            preact = full[c].astype(F32) + enc_bias[...]
            gating = jax.nn.sigmoid((preact - threshold[...]) * (1.0 / JUMP))
            value = preact * gating
            lat[c] = value.astype(BF)
            slope[c] = gating + value * (1.0 - gating) * (1.0 / JUMP)

        def to_preact_grad():
            for copy in grads_out(c):
                copy.start()
            lat[c] = (full[c].astype(F32) * slope[c]).astype(BF)

        def to_error():
            def then(total):
                row = lax.broadcasted_iota(jnp.int32, (ROWS, 1), 0)
                first = ((y * N + zh) * N + x) * ROWS
                keeps = jnp.zeros((ROWS, 1), jnp.int32)
                for i in range(ROWS):
                    keeps = jnp.where(row == i, mask[first + i], keeps)
                value = keeps.astype(F32) * (total + dec_bias[...] - acts[...].astype(F32))
                err[...] = value
                errh[...] = value.astype(BF)
                mean = jnp.sum(value * value, axis=1, keepdims=True) * (1.0 / depth)
                lane = lax.broadcasted_iota(jnp.int32, (ROWS, ROWS), 1)
                sq[...] = jnp.sum(jnp.where(row == lane, mean, 0.0), axis=0, keepdims=True)
                pltpu.make_async_copy(sq, sq_out, osem.at[C]).start()

            owned(then)
            z_send(errh)

        def to_input_grad():
            def then(total):
                ig[...] = (total - err[...]).astype(BF)

            wait_outs(c)
            owned(then)

        def dot(a, b, dims):
            return lax.dot_general(a, b, (dims, ((), ())), preferred_element_type=F32)

        def tokens():
            return ag[c].reshape(M, depth)

        def encode(lhs, where):
            return dot(lhs(), enc[:, where], ((1,), (0,)))

        def decode_back(lhs, where):
            return dot(lhs(), dec[where, :], ((1,), (1,)))

        def tiles(h):
            begin = 0
            while begin < half:
                length = min(512, half - begin)
                yield pl.ds(h * half + begin, length), length
                begin += length

        def decode(h):
            for where, length in tiles(h):
                value = dot(lat[c], dec[:, where], ((1,), (0,)))
                ps[c, :, :, :, where] = value.reshape(N, N, R, length).astype(BF)

        def encode_back(h):
            for where, length in tiles(h):
                value = dot(lat[c], enc[where, :], ((1,), (1,)))
                ps[c, :, :, :, where] = value.reshape(N, N, R, length).astype(BF)

        def wait_enc():
            if c == 0:
                enc_copy.wait()

        def wait_dec():
            if c == 0:
                for copy in (dec_copy, *small):
                    copy.wait()

        def joined(*parts):
            def run():
                for part in parts:
                    part()

            return run

        g1, l1, s1 = gather_stages(acts), layer_stages(tokens, encode, 256), scatter_stages(decode)
        g2, l2, s2 = gather_stages(errh), layer_stages(tokens, decode_back, 256), scatter_stages(encode_back)
        return [
            z_first,
            *g1[:-1],
            joined(g1[-1], wait_enc, l1[0]),
            *l1[1:-1],
            joined(l1[-1], wait_dec, to_latent, s1[0]),
            *s1[1:],
            to_error,
            *g2[:-1],
            joined(g2[-1], l2[0]),
            *l2[1:-1],
            joined(l2[-1], to_preact_grad, s2[0]),
            *s2[1:],
            to_input_grad,
        ]

    plans = [iter(chunk(c)) for c in range(C)]
    for c in TURNS:
        next(plans[c])()
    assert all(next(plan, None) is None for plan in plans)
    ig_copy = pltpu.make_async_copy(ig, ig_out, osem.at[C])
    ig_copy.start()
    ig_copy.wait()


def finish(sq_hbm, ig_hbm, lg_hbm, sq_out, ig_out, lg_out, sq, ig, raw, wide, isem, osem):
    parts = isem.shape[0] - 2
    length = raw.shape[0] // parts

    def rows(p):
        return pl.ds(p * length, length)

    ins = [pltpu.make_async_copy(lg_hbm.at[rows(p)], raw.at[rows(p)], isem.at[p]) for p in range(parts)]
    ins += [pltpu.make_async_copy(src, dst, isem.at[parts + n]) for n, (src, dst) in enumerate(((sq_hbm, sq), (ig_hbm, ig)))]
    outs = [pltpu.make_async_copy(wide.at[rows(p)], lg_out.at[rows(p)], osem.at[p]) for p in range(parts)]
    outs += [pltpu.make_async_copy(src, dst, osem.at[parts + n]) for n, (src, dst) in enumerate(((sq, sq_out), (ig, ig_out)))]
    for copy in ins:
        copy.start()
    for p in range(parts):
        ins[p].wait()
        wide[rows(p)] = raw[rows(p)].astype(F32)
        outs[p].start()
    for n in (parts, parts + 1):
        ins[n].wait()
        outs[n].start()
    for copy in outs:
        copy.wait()


def shards(activations, enc_weight, dec_weight, enc_bias, threshold, dec_bias, token_mask):
    depth, feats = enc_weight.shape[1:]
    half = depth // 2
    hbm = pl.BlockSpec(memory_space=pltpu.HBM)
    dma = pltpu.SemaphoreType.DMA
    scratch = [
        pltpu.VMEM((ROWS, depth), BF),
        *[pltpu.VMEM((1, feats), F32)] * 2,
        pltpu.VMEM((1, depth), F32),
        pltpu.SMEM(token_mask.shape, jnp.int32),
        pltpu.VMEM((depth, feats), BF),
        pltpu.VMEM((feats, depth), BF),
        pltpu.VMEM((C, N, N, R, depth), BF),
        pltpu.VMEM((C, S, ROWS, depth), BF),
        pltpu.VMEM((C, N, N, R, depth), BF),
        *[pltpu.VMEM((C, 2, N, R, half), BF)] * 3,
        pltpu.VMEM((C, 2, N, R, half), BF),
        *[pltpu.VMEM((C, 2, R, half), BF)] * 3,
        pltpu.VMEM((C, S, ROWS, depth), BF),
        pltpu.VMEM((N - 1, ROWS, depth), BF),
        pltpu.VMEM((C, HM, feats), F32),
        *[pltpu.VMEM((C, HM, feats), BF)] * 4,
        pltpu.VMEM((C, M, feats), BF),
        pltpu.VMEM((C, M, feats), BF),
        pltpu.VMEM((C, M, feats), F32),
        pltpu.VMEM((ROWS, depth), F32),
        pltpu.VMEM((ROWS, depth), BF),
        pltpu.VMEM((1, ROWS), F32),
        pltpu.VMEM((ROWS, depth), BF),
        dma((7,)),
        dma((C + 1,)),
        dma((3,)), dma((C, S)),
        dma((C, 2, 2, 6)), dma((C, 2, 2, 6)),
        dma((C, 2, 2, 6)), dma((C, 2, 2, 6)),
        dma((C, S)), dma((3,)),
        dma((C, 3, PIECES)), dma((C, 3, PIECES)),
    ]
    sq, ig, lg = pl.pallas_call(
        kernel,
        out_shape=(
            jax.ShapeDtypeStruct((1, ROWS), F32),
            jax.ShapeDtypeStruct((ROWS, depth), BF),
            jax.ShapeDtypeStruct((N * N * N * ROWS, feats), BF),
        ),
        in_specs=[hbm] * 7,
        out_specs=(hbm,) * 3,
        scratch_shapes=scratch,
        compiler_params=pltpu.CompilerParams(
            collective_id=0, has_side_effects=True, vmem_limit_bytes=67043328
        ),
    )(
        activations[:, 0], enc_weight[0], dec_weight[0], enc_bias[None], threshold[None], dec_bias, token_mask,
    )
    tokens, parts = N * N * N * ROWS, 4
    sq, ig, lg = pl.pallas_call(
        finish,
        out_shape=(
            jax.ShapeDtypeStruct((1, ROWS), F32),
            jax.ShapeDtypeStruct((ROWS, depth), BF),
            jax.ShapeDtypeStruct((tokens, feats), F32),
        ),
        in_specs=[hbm] * 3,
        out_specs=(hbm,) * 3,
        scratch_shapes=[
            pltpu.VMEM((1, ROWS), F32),
            pltpu.VMEM((ROWS, depth), BF),
            pltpu.VMEM((tokens, feats), BF),
            pltpu.VMEM((tokens, feats), F32),
            dma((parts + 2,)), dma((parts + 2,)),
        ],
        compiler_params=pltpu.CompilerParams(vmem_limit_bytes=67043328),
    )(sq, ig, lg)
    return sq.reshape(ROWS, 1), lg, ig[:, None]


def solution(mesh):
    finer = Mesh(mesh.devices.reshape(2, 2, N, N, N), LAYER + FEAT)
    return jax.shard_map(
        shards,
        mesh=finer,
        in_specs=(
            P(FEAT, LAYER, None),
            P(LAYER, None, FEAT),
            P(LAYER, FEAT, None),
            P(FEAT),
            P(FEAT),
            P(LAYER, None),
            P(),
        ),
        out_specs=(P(FEAT, LAYER), P(None, FEAT), P(FEAT, LAYER, None)),
        check_vma=False,
    )
```

```python
import functools

import jax
import jax.numpy as jnp
from jax import lax
from jax.experimental import pallas as pl
from jax.experimental.pallas import tpu as pltpu
from jax.sharding import Mesh
from jax.sharding import PartitionSpec as P

FEAT = ("y", "zh", "x")
LAYER = ("zl", "co")
MESH = pl.DeviceIdType.MESH
BF = jnp.bfloat16
F32 = jnp.float32
JUMP = 0.25

N = 4
C = 4
S = N // C
ROWS = 8
R = S * ROWS
M = N * N * R
HM = M // 2
PIECES = 2
TURNS = (
    0, 2, 3, 1, 0, 2, 4, 3, 0, 2, 4, 0, 1, 2, 3, 0, 0, 1, 0, 2, 2, 3, 0, 2, 0, 2, 3, 1, 0, 3,
    3, 0, 3, 2, 2, 1, 1, 2, 1, 1, 3, 3, 0, 2, 3, 0, 1, 1, 2, 1, 3, 0, 1, 2, 3, 0, 1, 2, 3, 1,
    0, 2, 3, 0, 1, 2, 3, 0, 1, 2, 3, 0, 0, 1, 0, 0, 2, 3, 2, 2, 1, 0, 2, 3, 3, 3, 0, 1, 1, 3,
    2, 0, 2, 1, 1, 2, 3, 3, 0, 3, 1, 1, 2, 1, 3, 1, 0, 2, 3, 1, 2, 0, 3, 1, 3, 0, 2, 1,
)


def kernel(
    acts_hbm, enc_hbm, dec_hbm, enc_bias_hbm, threshold_hbm, dec_bias_hbm, mask_hbm,
    sq_out, ig_out, lg_out,
    acts, enc_bias, threshold, dec_bias, mask, enc, dec, enc_t, dec_t, ag, zbuf, ps, r1, ps2, r2, ps3, zr,
    keep, dsend, drecv, zs, zv, full, lat, slope, err, errh, sq, ig,
    wsem, osem, zsnd, zrcv, snd, gn, gw, sw, sn, zrsnd, zrrcv, lsnd, lrcv,
):
    depth = ag.shape[-1]
    feats = lat.shape[-1]
    half = depth // 2
    cut = (half // 256 + 1) * 128
    x, y, zh = lax.axis_index("x"), lax.axis_index("y"), lax.axis_index("zh")
    zl, co = lax.axis_index("zl"), lax.axis_index("co")
    at = {"x": x, "y": y, "zh": zh}

    def step(axis, by):
        return lax.rem(at[axis] + (by + N) % N, N)

    def to(axis, by):
        return {axis: step(axis, by)}

    acts_copy, enc_copy, dec_copy, *small = [
        pltpu.make_async_copy(src, dst, wsem.at[n])
        for n, (src, dst) in enumerate((
            (acts_hbm, acts), (enc_hbm, enc), (dec_hbm, dec), (enc_bias_hbm, enc_bias),
            (threshold_hbm, threshold), (dec_bias_hbm, dec_bias), (mask_hbm, mask),
        ))
    ]
    for copy in (acts_copy, *small, enc_copy, dec_copy):
        copy.start()

    barrier = pltpu.get_barrier_semaphore()
    peers = [to(axis, by) for axis in ("x", "y", "zh") for by in (1, 2, 3)]
    peers += [{"zl": 1 - zl}, {"co": 1 - co}]
    for peer in peers:
        pl.semaphore_signal(barrier, inc=1, device_id=peer, device_id_type=MESH)
    pl.semaphore_wait(barrier, len(peers))
    acts_copy.wait()

    def remote(src, dst, send, recv, peer):
        return pltpu.make_async_remote_copy(
            src_ref=src, dst_ref=dst, send_sem=send, recv_sem=recv,
            device_id=peer, device_id_type=MESH,
        )

    def cols(h, part):
        base, length = {None: (0, half), 0: (0, cut), 1: (cut, half - cut)}[part]
        return pl.ds(h * half + base, length)

    class Ring:
        def __init__(self, axis, block, size, send, recv):
            self.axis, self.block, self.size, self.send, self.recv = axis, block, size, send, recv
            self.copies = []

        def push(self, src, dst, by):
            recv = self.recv.at[min(len(self.copies), self.recv.shape[0] - 1)]
            copy = remote(src, dst, self.send, recv, to(self.axis, by))
            copy.start()
            self.copies.append(copy)

        def wait(self, blocks, sem):
            ref = self.size.at[pl.ds(0, blocks)]
            pltpu.make_async_copy(ref, ref, sem).wait()

        def first(self, n):
            self.copies[n].wait_recv()

        def rest(self):
            last = self.recv.shape[0] - 1
            self.wait(3 if last == 0 else 2, self.recv.at[last])

        def sent(self):
            self.wait(3, self.send)

    class Gather(Ring):
        def pass_on(self, pos, part, by):
            ref = self.block(pos, part)
            self.push(ref, ref, by)

        def start(self):
            me = at[self.axis]
            self.pass_on(me, 0, 1)
            self.pass_on(me, 1, -1)
            self.pass_on(me, 1, 1)
            self.pass_on(me, 0, -1)

        def middle(self):
            self.first(0)
            self.pass_on(step(self.axis, -1), 0, 1)
            self.first(1)
            self.pass_on(step(self.axis, 1), 1, -1)

        def finish(self):
            self.rest()
            self.sent()

    class DirectGather(Ring):
        def start(self):
            ref = self.block(at[self.axis], None)
            for by in (2, 1, -1):
                self.push(ref, ref, by)

        def finish(self):
            self.rest()
            self.sent()

    class Scatter(Ring):
        def __init__(self, axis, block, size, send, recv):
            super().__init__(axis, block, size, send, recv)
            self.f, self.a, self.b = (size.at[n] for n in range(3))

        def slot(self, buf, part):
            return buf.at[(slice(None),) * (len(buf.shape) - 1) + (cols(0, part),)]

        def start(self):
            far = step(self.axis, 2)
            self.push(self.block(far, 0), self.slot(self.f, 0), 1)
            self.push(self.block(far, 1), self.slot(self.f, 1), -1)
            self.push(self.block(step(self.axis, 1), 1), self.slot(self.a, 1), 1)
            self.push(self.block(step(self.axis, -1), 0), self.slot(self.b, 0), -1)

        def middle(self):
            for part, by, into in ((0, 1, self.a), (1, -1, self.b)):
                self.first(part)
                here = self.slot(self.f, part)
                own = self.block(step(self.axis, by), part)
                here[...] = (here[...].astype(F32) + own[...].astype(F32)).astype(BF)
                self.push(here, self.slot(into, part), by)

        def finish(self):
            self.rest()
            total = self.block(at[self.axis], None)[...].astype(F32)
            total = total + self.a[...].astype(F32) + self.b[...].astype(F32)
            self.sent()
            return total

    class DirectScatter(Scatter):
        def start(self):
            for by, into in ((2, self.f), (1, self.a), (-1, self.b)):
                self.push(self.block(step(self.axis, by), None), into, by)

        def finish(self):
            self.rest()
            total = self.block(at[self.axis], None)[...].astype(F32) + self.f[...].astype(F32)
            total = total + self.a[...].astype(F32) + self.b[...].astype(F32)
            self.sent()
            return total

    def grads_out(c):
        for j in range(M // ROWS):
            row = ((j // (N * S) * N + c * S + j % S) * N + j // S % N) * ROWS
            yield pltpu.make_async_copy(full.at[c, pl.ds(j * ROWS, ROWS)], lg_out.at[pl.ds(row, ROWS)], osem.at[c])

    def wait_outs(c):
        pltpu.make_async_copy(full.at[c], lg_out.at[pl.ds(0, M)], osem.at[c]).wait()

        @pl.when(zh // S == c)
        def _():
            pltpu.make_async_copy(sq, sq_out, osem.at[C]).wait()

    def chunk(c):
        def z_send(src):
            for s in range(S):
                @pl.when(zh == c * S + s)
                def _():
                    zbuf[c, s] = src[...]
                    for k in (1, 2, 3):
                        remote(src, zbuf.at[c, s], zsnd.at[k - 1], zrcv.at[c, s], to("zh", k)).start()

        def z_wait(src):
            for s in range(S):
                one = remote(src, zbuf.at[c, s], zsnd.at[0], zrcv.at[c, s], to("zh", 1))

                @pl.when(zh != c * S + s)
                def _():
                    one.wait_recv()

                @pl.when(zh == c * S + s)
                def _():
                    for k in (1, 2, 3):
                        remote(src, zbuf.at[c, s], zsnd.at[k - 1], zrcv.at[c, s], to("zh", k)).wait_send()

            ag[c, y, x] = zbuf[c].astype(F32).reshape(R, depth).astype(BF)

        def gather_stages(src):
            near = [
                DirectGather("x", lambda i, p: ag.at[c, y, i, :, cols(0, p)], r2.at[c, 0], snd.at[c, 0], gn.at[c, 0]),
                DirectGather("y", lambda i, p: ag.at[c, i, x, :, cols(1, p)], r2.at[c, 1], snd.at[c, 1], gn.at[c, 1]),
            ]
            wide = [
                Gather("y", lambda i, p: ag.at[c, i, :, :, cols(0, p)], r1.at[c, 0], snd.at[c, 0], gw.at[c, 0]),
                Gather("x", lambda i, p: ag.at[c, :, i, :, cols(1, p)], r1.at[c, 1], snd.at[c, 1], gw.at[c, 1]),
            ]

            def begin():
                z_wait(src)
                for g in near:
                    g.start()

            def widen():
                for g, w in zip(near, wide):
                    g.finish()
                    w.start()

            def forward():
                for w in wide:
                    w.middle()

            def end():
                for w in wide:
                    w.finish()

            return [begin, widen, forward, end]

        def layer_stages(lhs, product):
            copies = {}
            width = feats // PIECES

            def exchange(kind, p, src, dst, peer):
                copies[kind, p] = remote(src, dst, lsnd.at[c, p], lrcv.at[c, kind, p], peer)
                copies[kind, p].start()

            def multiply(p):
                piece = pl.ds(p * width, width)
                value = product(lhs, piece)
                low, high = value[:HM], value[HM:]
                keep[c, :, piece] = jnp.where(co == 0, low, high)
                dsend[c, :, piece] = jnp.where(co == 0, high, low).astype(BF)
                exchange(0, p, dsend.at[c, :, piece], drecv.at[c, :, piece], {"co": 1 - co})

            def pair(p):
                copies[0, p].wait()
                piece = pl.ds(p * width, width)
                zs[c, :, piece] = (keep[c, :, piece] + drecv[c, :, piece].astype(F32)).astype(BF)
                exchange(1, p, zs.at[c, :, piece], zv.at[c, :, piece], {"zl": 1 - zl})

            def share(p):
                copies[1, p].wait()
                piece = pl.ds(p * width, width)
                mine = pl.ds(pl.multiple_of(co * HM, HM), HM)
                full[c, mine, piece] = (zs[c, :, piece].astype(F32) + zv[c, :, piece].astype(F32)).astype(BF)
                ref = full.at[c, mine, piece]
                exchange(2, p, ref, ref, {"co": 1 - co})

            def end():
                for p in range(PIECES):
                    copies[2, p].wait()

            pieces = range(PIECES)
            return [
                *[functools.partial(multiply, p) for p in pieces],
                *[functools.partial(pair, p) for p in pieces],
                *[functools.partial(share, p) for p in pieces],
                end,
            ]

        def scatter_stages(multiply):
            wide = [
                Scatter("y", lambda i, p: ps.at[c, i, :, :, cols(0, p)], r1.at[c, 0], snd.at[c, 0], sw.at[c, 0]),
                Scatter("x", lambda i, p: ps.at[c, :, i, :, cols(1, p)], r1.at[c, 1], snd.at[c, 1], sw.at[c, 1]),
            ]
            near = [
                DirectScatter(axis, lambda i, p, h=h: ps2.at[c, h, i, :, cols(0, p)], r2.at[c, h], snd.at[c, h], sn.at[c, h])
                for h, axis in enumerate(("x", "y"))
            ]

            def begin():
                for h in range(2):
                    multiply(h)
                    wide[h].start()

            def forward():
                for w in wide:
                    w.middle()

            def narrow():
                for h in range(2):
                    ps2[c, h] = wide[h].finish().astype(BF)
                    near[h].start()

            def z_out():
                for h in range(2):
                    ps3[c, :, :, cols(h, None)] = near[h].finish().reshape(S, ROWS, half).astype(BF)
                for s in range(S):
                    @pl.when(zh != c * S + s)
                    def _():
                        k = lax.rem(zh - (c * S + s) + N, N) - 1
                        remote(ps3.at[c, s], zr.at[k], zrsnd.at[c, s], zrrcv.at[k], {"zh": c * S + s}).start()

            return [begin, forward, narrow, z_out]

        def owned(then):
            for s in range(S):
                @pl.when(zh != c * S + s)
                def _():
                    remote(ps3.at[c, s], zr.at[0], zrsnd.at[c, s], zrrcv.at[0], {"zh": c * S + s}).wait_send()

                @pl.when(zh == c * S + s)
                def _():
                    total = ps3[c, s].astype(F32)
                    for k in range(3):
                        remote(ps3.at[c, s], zr.at[k], zrsnd.at[c, s], zrrcv.at[k], to("zh", 1)).wait_recv()
                        total = total + zr[k].astype(F32)
                    then(total)

        def z_first():
            z_send(acts)

        def to_latent():
            preact = full[c].astype(F32) + enc_bias[...]
            gating = jax.nn.sigmoid((preact - threshold[...]) * (1.0 / JUMP))
            value = preact * gating
            lat[c] = value.astype(BF)
            slope[c] = gating + value * (1.0 - gating) * (1.0 / JUMP)

        def to_preact_grad():
            for copy in grads_out(c):
                copy.start()
            lat[c] = (full[c].astype(F32) * slope[c]).astype(BF)

        def to_error():
            def then(total):
                row = lax.broadcasted_iota(jnp.int32, (ROWS, 1), 0)
                first = ((y * N + zh) * N + x) * ROWS
                keeps = jnp.zeros((ROWS, 1), jnp.int32)
                for i in range(ROWS):
                    keeps = jnp.where(row == i, mask[first + i], keeps)
                value = keeps.astype(F32) * (total + dec_bias[...] - acts[...].astype(F32))
                err[...] = value
                errh[...] = value.astype(BF)
                mean = jnp.sum(value * value, axis=1, keepdims=True) * (1.0 / depth)
                lane = lax.broadcasted_iota(jnp.int32, (ROWS, ROWS), 1)
                sq[...] = jnp.sum(jnp.where(row == lane, mean, 0.0), axis=0, keepdims=True)
                pltpu.make_async_copy(sq, sq_out, osem.at[C]).start()

            owned(then)
            z_send(errh)

        def to_input_grad():
            def then(total):
                ig[...] = (total - err[...]).astype(BF)

            wait_outs(c)
            owned(then)

        def dot(a, b):
            return jnp.dot(a, b, preferred_element_type=F32)

        def tokens():
            return ag[c].reshape(M, depth)

        def encode(lhs, where):
            return dot(lhs(), enc[:, where])

        def decode_back(lhs, where):
            return dot(lhs(), dec_t[:, where])

        def tiles(h):
            begin = 0
            while begin < half:
                length = min(512, half - begin)
                yield pl.ds(h * half + begin, length), length
                begin += length

        def decode(h):
            for where, length in tiles(h):
                value = dot(lat[c], dec[:, where])
                ps[c, :, :, :, where] = value.reshape(N, N, R, length).astype(BF)

        def encode_back(h):
            for where, length in tiles(h):
                value = dot(lat[c], enc_t[:, where])
                ps[c, :, :, :, where] = value.reshape(N, N, R, length).astype(BF)

        def joined(*parts):
            def run():
                for part in parts:
                    part()

            return run

        g1, l1, s1 = gather_stages(acts), layer_stages(tokens, encode), scatter_stages(decode)
        g2, l2, s2 = gather_stages(errh), layer_stages(tokens, decode_back), scatter_stages(encode_back)
        return [
            z_first,
            *g1[:-1],
            joined(g1[-1], l1[0]),
            *l1[1:-1],
            joined(l1[-1], to_latent, s1[0]),
            *s1[1:],
            to_error,
            *g2[:-1],
            joined(g2[-1], l2[0]),
            *l2[1:-1],
            joined(l2[-1], to_preact_grad, s2[0]),
            *s2[1:],
            to_input_grad,
        ]

    def turned(copies, src, dst):
        for copy in copies:
            copy.wait()

        def one(j, carry):
            where = pl.ds(pl.multiple_of(j * 256, 256), 256)
            dst[:, where] = src[where, :].T
            return carry

        lax.fori_loop(0, src.shape[0] // 256, one, 0)

    weights = [
        functools.partial(turned, [enc_copy], enc, enc_t),
        functools.partial(turned, [dec_copy, *small], dec, dec_t),
    ]
    plans = [iter(chunk(c)) for c in range(C)] + [iter(weights)]
    for c in TURNS:
        next(plans[c])()
    assert all(next(plan, None) is None for plan in plans)
    ig_copy = pltpu.make_async_copy(ig, ig_out, osem.at[C])
    ig_copy.start()
    ig_copy.wait()


def finish(sq_hbm, ig_hbm, lg_hbm, sq_out, ig_out, lg_out, sq, ig, raw, wide, isem, osem):
    parts = isem.shape[0] - 2
    length = raw.shape[0] // parts

    def rows(p):
        return pl.ds(p * length, length)

    ins = [pltpu.make_async_copy(lg_hbm.at[rows(p)], raw.at[rows(p)], isem.at[p]) for p in range(parts)]
    ins += [pltpu.make_async_copy(src, dst, isem.at[parts + n]) for n, (src, dst) in enumerate(((sq_hbm, sq), (ig_hbm, ig)))]
    outs = [pltpu.make_async_copy(wide.at[rows(p)], lg_out.at[rows(p)], osem.at[p]) for p in range(parts)]
    outs += [pltpu.make_async_copy(src, dst, osem.at[parts + n]) for n, (src, dst) in enumerate(((sq, sq_out), (ig, ig_out)))]
    for copy in ins:
        copy.start()
    for p in range(parts):
        ins[p].wait()
        wide[rows(p)] = raw[rows(p)].astype(F32)
        outs[p].start()
    for n in (parts, parts + 1):
        ins[n].wait()
        outs[n].start()
    for copy in outs:
        copy.wait()


def shards(activations, enc_weight, dec_weight, enc_bias, threshold, dec_bias, token_mask):
    depth, feats = enc_weight.shape[1:]
    half = depth // 2
    hbm = pl.BlockSpec(memory_space=pltpu.HBM)
    dma = pltpu.SemaphoreType.DMA
    scratch = [
        pltpu.VMEM((ROWS, depth), BF),
        *[pltpu.VMEM((1, feats), F32)] * 2,
        pltpu.VMEM((1, depth), F32),
        pltpu.SMEM(token_mask.shape, jnp.int32),
        pltpu.VMEM((depth, feats), BF),
        pltpu.VMEM((feats, depth), BF),
        pltpu.VMEM((feats, depth), BF),
        pltpu.VMEM((depth, feats), BF),
        pltpu.VMEM((C, N, N, R, depth), BF),
        pltpu.VMEM((C, S, ROWS, depth), BF),
        pltpu.VMEM((C, N, N, R, depth), BF),
        pltpu.VMEM((C, 2, 3, N, R, half), BF),
        pltpu.VMEM((C, 2, N, R, half), BF),
        pltpu.VMEM((C, 2, 3, R, half), BF),
        pltpu.VMEM((C, S, ROWS, depth), BF),
        pltpu.VMEM((N - 1, ROWS, depth), BF),
        pltpu.VMEM((C, HM, feats), F32),
        *[pltpu.VMEM((C, HM, feats), BF)] * 4,
        pltpu.VMEM((C, M, feats), BF),
        pltpu.VMEM((C, M, feats), BF),
        pltpu.VMEM((C, M, feats), F32),
        pltpu.VMEM((ROWS, depth), F32),
        pltpu.VMEM((ROWS, depth), BF),
        pltpu.VMEM((1, ROWS), F32),
        pltpu.VMEM((ROWS, depth), BF),
        dma((7,)),
        dma((C + 1,)),
        dma((3,)), dma((C, S)),
        dma((C, 2)),
        dma((C, 2, 1)), dma((C, 2, 3)), dma((C, 2, 3)), dma((C, 2, 1)),
        dma((C, S)), dma((3,)),
        dma((C, PIECES)), dma((C, 3, PIECES)),
    ]
    sq, ig, lg = pl.pallas_call(
        kernel,
        out_shape=(
            jax.ShapeDtypeStruct((1, ROWS), F32),
            jax.ShapeDtypeStruct((ROWS, depth), BF),
            jax.ShapeDtypeStruct((N * N * N * ROWS, feats), BF),
        ),
        in_specs=[hbm] * 7,
        out_specs=(hbm,) * 3,
        scratch_shapes=scratch,
        compiler_params=pltpu.CompilerParams(
            collective_id=0, has_side_effects=True, vmem_limit_bytes=67043328
        ),
    )(
        activations[:, 0], enc_weight[0], dec_weight[0], enc_bias[None], threshold[None], dec_bias, token_mask,
    )
    tokens, parts = N * N * N * ROWS, 4
    sq, ig, lg = pl.pallas_call(
        finish,
        out_shape=(
            jax.ShapeDtypeStruct((1, ROWS), F32),
            jax.ShapeDtypeStruct((ROWS, depth), BF),
            jax.ShapeDtypeStruct((tokens, feats), F32),
        ),
        in_specs=[hbm] * 3,
        out_specs=(hbm,) * 3,
        scratch_shapes=[
            pltpu.VMEM((1, ROWS), F32),
            pltpu.VMEM((ROWS, depth), BF),
            pltpu.VMEM((tokens, feats), BF),
            pltpu.VMEM((tokens, feats), F32),
            dma((parts + 2,)), dma((parts + 2,)),
        ],
        compiler_params=pltpu.CompilerParams(vmem_limit_bytes=67043328),
    )(sq, ig, lg)
    return sq.reshape(ROWS, 1), lg, ig[:, None]


def solution(mesh):
    finer = Mesh(mesh.devices.reshape(2, 2, N, N, N), LAYER + FEAT)
    return jax.shard_map(
        shards,
        mesh=finer,
        in_specs=(
            P(FEAT, LAYER, None),
            P(LAYER, None, FEAT),
            P(LAYER, FEAT, None),
            P(FEAT),
            P(FEAT),
            P(LAYER, None),
            P(),
        ),
        out_specs=(P(FEAT, LAYER), P(None, FEAT), P(FEAT, LAYER, None)),
        check_vma=False,
    )
```

```python
import functools

import jax
import jax.numpy as jnp
from jax import lax
from jax.experimental import pallas as pl
from jax.experimental.pallas import tpu as pltpu
from jax.sharding import Mesh
from jax.sharding import PartitionSpec as P

FEAT = ("y", "zh", "x")
LAYER = ("zl", "co")
MESH = pl.DeviceIdType.MESH
BF = jnp.bfloat16
F32 = jnp.float32
JUMP = 0.25

N = 4
C = 4
S = N // C
ROWS = 8
R = S * ROWS
M = N * N * R
HM = M // 2
PIECES = 2
TURNS = (
    0, 2, 3, 1, 0, 2, 4, 3, 0, 2, 4, 0, 1, 2, 3, 0, 0, 1, 0, 2, 2, 3, 0, 2, 0, 2, 3, 1, 0, 3,
    3, 0, 3, 2, 2, 1, 1, 2, 1, 1, 3, 3, 0, 2, 3, 0, 1, 1, 2, 1, 3, 0, 1, 2, 3, 0, 1, 2, 3, 1,
    0, 2, 3, 0, 1, 2, 3, 0, 1, 2, 3, 0, 0, 1, 0, 0, 2, 3, 2, 2, 1, 0, 2, 3, 3, 3, 0, 1, 1, 3,
    2, 0, 2, 1, 1, 2, 3, 3, 0, 3, 1, 1, 2, 1, 3, 1, 0, 2, 3, 1, 2, 0, 3, 1, 3, 0, 2, 1,
)


def kernel(
    acts_hbm, enc_hbm, dec_hbm, enc_bias_hbm, threshold_hbm, dec_bias_hbm, mask_hbm,
    sq_out, ig_out, lg_out,
    acts, enc_bias, threshold, dec_bias, mask, enc, dec, enc_t, dec_t, ag, zbuf, ps, r1, ps2, r2, ps3, zr,
    keep, dsend, drecv, zs, zv, full, lat, slope, err, errh, sq, ig,
    wsem, osem, zsnd, zrcv, snd, gn, gw, sw, sn, zrsnd, zrrcv, lsnd, lrcv,
):
    depth = ag.shape[-1]
    feats = lat.shape[-1]
    half = depth // 2
    cut = (half // 256 + 1) * 128
    x, y, zh = lax.axis_index("x"), lax.axis_index("y"), lax.axis_index("zh")
    zl, co = lax.axis_index("zl"), lax.axis_index("co")
    at = {"x": x, "y": y, "zh": zh}

    def step(axis, by):
        return lax.rem(at[axis] + (by + N) % N, N)

    def to(axis, by):
        return {axis: step(axis, by)}

    acts_copy, enc_copy, dec_copy, *small = [
        pltpu.make_async_copy(src, dst, wsem.at[n])
        for n, (src, dst) in enumerate((
            (acts_hbm, acts), (enc_hbm, enc), (dec_hbm, dec), (enc_bias_hbm, enc_bias),
            (threshold_hbm, threshold), (dec_bias_hbm, dec_bias), (mask_hbm, mask),
        ))
    ]
    for copy in (acts_copy, *small, enc_copy, dec_copy):
        copy.start()

    barrier = pltpu.get_barrier_semaphore()
    peers = [to(axis, by) for axis in ("x", "y", "zh") for by in (1, 2, 3)]
    peers += [{"zl": 1 - zl}, {"co": 1 - co}]
    for peer in peers:
        pl.semaphore_signal(barrier, inc=1, device_id=peer, device_id_type=MESH)
    pl.semaphore_wait(barrier, len(peers))
    acts_copy.wait()

    def remote(src, dst, send, recv, peer):
        return pltpu.make_async_remote_copy(
            src_ref=src, dst_ref=dst, send_sem=send, recv_sem=recv,
            device_id=peer, device_id_type=MESH,
        )

    def cols(h, part):
        base, length = {None: (0, half), 0: (0, cut), 1: (cut, half - cut)}[part]
        return pl.ds(h * half + base, length)

    class Ring:
        def __init__(self, axis, block, size, send, recv):
            self.axis, self.block, self.size, self.send, self.recv = axis, block, size, send, recv
            self.copies = []

        def push(self, src, dst, by):
            recv = self.recv.at[min(len(self.copies), self.recv.shape[0] - 1)]
            copy = remote(src, dst, self.send, recv, to(self.axis, by))
            copy.start()
            self.copies.append(copy)

        def wait(self, blocks, sem):
            ref = self.size.at[pl.ds(0, blocks)]
            pltpu.make_async_copy(ref, ref, sem).wait()

        def first(self, n):
            self.copies[n].wait_recv()

        def rest(self):
            last = self.recv.shape[0] - 1
            self.wait(3 if last == 0 else 2, self.recv.at[last])

        def sent(self):
            self.wait(3, self.send)

    class Gather(Ring):
        def pass_on(self, pos, part, by):
            ref = self.block(pos, part)
            self.push(ref, ref, by)

        def start(self):
            me = at[self.axis]
            self.pass_on(me, 0, 1)
            self.pass_on(me, 1, -1)
            self.pass_on(me, 1, 1)
            self.pass_on(me, 0, -1)

        def middle(self):
            self.first(0)
            self.pass_on(step(self.axis, -1), 0, 1)
            self.first(1)
            self.pass_on(step(self.axis, 1), 1, -1)

        def finish(self):
            self.rest()
            self.sent()

    class DirectGather(Ring):
        def start(self):
            ref = self.block(at[self.axis], None)
            for by in (2, 1, -1):
                self.push(ref, ref, by)

        def finish(self):
            self.rest()
            self.sent()

    class Scatter(Ring):
        def __init__(self, axis, block, size, send, recv):
            super().__init__(axis, block, size, send, recv)
            self.f, self.a, self.b = (size.at[n] for n in range(3))

        def slot(self, buf, part):
            return buf.at[(slice(None),) * (len(buf.shape) - 1) + (cols(0, part),)]

        def start(self):
            far = step(self.axis, 2)
            self.push(self.block(far, 0), self.slot(self.f, 0), 1)
            self.push(self.block(far, 1), self.slot(self.f, 1), -1)
            self.push(self.block(step(self.axis, 1), 1), self.slot(self.a, 1), 1)
            self.push(self.block(step(self.axis, -1), 0), self.slot(self.b, 0), -1)

        def middle(self):
            for part, by, into in ((0, 1, self.a), (1, -1, self.b)):
                self.first(part)
                here = self.slot(self.f, part)
                own = self.block(step(self.axis, by), part)
                here[...] = (here[...].astype(F32) + own[...].astype(F32)).astype(BF)
                self.push(here, self.slot(into, part), by)

        def finish(self):
            self.rest()
            total = self.block(at[self.axis], None)[...].astype(F32)
            total = total + self.a[...].astype(F32) + self.b[...].astype(F32)
            self.sent()
            return total

    class DirectScatter(Scatter):
        def start(self):
            for by, into in ((2, self.f), (1, self.a), (-1, self.b)):
                self.push(self.block(step(self.axis, by), None), into, by)

        def finish(self):
            self.rest()
            total = self.block(at[self.axis], None)[...].astype(F32) + self.f[...].astype(F32)
            total = total + self.a[...].astype(F32) + self.b[...].astype(F32)
            self.sent()
            return total

    def grads_out(c):
        for j in range(M // ROWS):
            row = ((j // (N * S) * N + c * S + j % S) * N + j // S % N) * ROWS
            yield pltpu.make_async_copy(full.at[c, pl.ds(j * ROWS, ROWS)], lg_out.at[pl.ds(row, ROWS)], osem.at[c])

    def wait_outs(c):
        pltpu.make_async_copy(full.at[c], lg_out.at[pl.ds(0, M)], osem.at[c]).wait()

        @pl.when(zh // S == c)
        def _():
            pltpu.make_async_copy(sq, sq_out, osem.at[C]).wait()

    def chunk(c):
        def z_send(src):
            for s in range(S):
                @pl.when(zh == c * S + s)
                def _():
                    zbuf[c, s] = src[...]
                    for k in (1, 2, 3):
                        remote(src, zbuf.at[c, s], zsnd.at[k - 1], zrcv.at[c, s], to("zh", k)).start()

        def z_wait(src):
            for s in range(S):
                one = remote(src, zbuf.at[c, s], zsnd.at[0], zrcv.at[c, s], to("zh", 1))

                @pl.when(zh != c * S + s)
                def _():
                    one.wait_recv()

                @pl.when(zh == c * S + s)
                def _():
                    for k in (1, 2, 3):
                        remote(src, zbuf.at[c, s], zsnd.at[k - 1], zrcv.at[c, s], to("zh", k)).wait_send()

            ag[c, y, x] = zbuf[c].astype(F32).reshape(R, depth).astype(BF)

        def gather_stages(src):
            near = [
                DirectGather("x", lambda i, p: ag.at[c, y, i, :, cols(0, p)], r2.at[c, 0], snd.at[c, 0], gn.at[c, 0]),
                DirectGather("y", lambda i, p: ag.at[c, i, x, :, cols(1, p)], r2.at[c, 1], snd.at[c, 1], gn.at[c, 1]),
            ]
            wide = [
                Gather("y", lambda i, p: ag.at[c, i, :, :, cols(0, p)], r1.at[c, 0], snd.at[c, 0], gw.at[c, 0]),
                Gather("x", lambda i, p: ag.at[c, :, i, :, cols(1, p)], r1.at[c, 1], snd.at[c, 1], gw.at[c, 1]),
            ]

            def begin():
                z_wait(src)
                for g in near:
                    g.start()

            def widen():
                for g, w in zip(near, wide):
                    g.finish()
                    w.start()

            def forward():
                for w in wide:
                    w.middle()

            def end():
                for w in wide:
                    w.finish()

            return [begin, widen, forward, end]

        def layer_stages(turn, lhs, product):
            copies = {}
            width = feats // PIECES

            def exchange(kind, p, src, dst, peer):
                copies[kind, p] = remote(src, dst, lsnd.at[c, p], lrcv.at[c, 3 if kind == 1 and turn else kind, p], peer)
                copies[kind, p].start()

            def multiply(p):
                piece = pl.ds(p * width, width)
                value = product(lhs, piece)
                low, high = value[:HM], value[HM:]
                keep[c, :, piece] = jnp.where(co == 0, low, high)
                dsend[c, :, piece] = jnp.where(co == 0, high, low).astype(BF)
                exchange(0, p, dsend.at[c, :, piece], drecv.at[c, :, piece], {"co": 1 - co})

            def pair(p):
                copies[0, p].wait()
                piece = pl.ds(p * width, width)
                zs[c, :, piece] = (keep[c, :, piece] + drecv[c, :, piece].astype(F32)).astype(BF)
                exchange(1, p, zs.at[c, :, piece], zv.at[turn, c, :, piece], {"zl": 1 - zl})

            def share(p):
                copies[1, p].wait()
                piece = pl.ds(p * width, width)
                mine = pl.ds(pl.multiple_of(co * HM, HM), HM)
                full[c, mine, piece] = (zs[c, :, piece].astype(F32) + zv[turn, c, :, piece].astype(F32)).astype(BF)
                ref = full.at[c, mine, piece]
                exchange(2, p, ref, ref, {"co": 1 - co})

            def end():
                for p in range(PIECES):
                    copies[2, p].wait()

            pieces = range(PIECES)
            return [
                *[functools.partial(multiply, p) for p in pieces],
                *[functools.partial(pair, p) for p in pieces],
                *[functools.partial(share, p) for p in pieces],
                end,
            ]

        def scatter_stages(multiply):
            wide = [
                Scatter("y", lambda i, p: ps.at[c, i, :, :, cols(0, p)], r1.at[c, 0], snd.at[c, 0], sw.at[c, 0]),
                Scatter("x", lambda i, p: ps.at[c, :, i, :, cols(1, p)], r1.at[c, 1], snd.at[c, 1], sw.at[c, 1]),
            ]
            near = [
                DirectScatter(axis, lambda i, p, h=h: ps2.at[c, h, i, :, cols(0, p)], r2.at[c, h], snd.at[c, h], sn.at[c, h])
                for h, axis in enumerate(("x", "y"))
            ]

            def begin():
                for h in range(2):
                    multiply(h)
                    wide[h].start()

            def forward():
                for w in wide:
                    w.middle()

            def narrow():
                for h in range(2):
                    ps2[c, h] = wide[h].finish().astype(BF)
                    near[h].start()

            def z_out():
                for h in range(2):
                    ps3[c, :, :, cols(h, None)] = near[h].finish().reshape(S, ROWS, half).astype(BF)
                for s in range(S):
                    @pl.when(zh != c * S + s)
                    def _():
                        k = lax.rem(zh - (c * S + s) + N, N) - 1
                        remote(ps3.at[c, s], zr.at[k], zrsnd.at[c, s], zrrcv.at[k], {"zh": c * S + s}).start()

            return [begin, forward, narrow, z_out]

        def owned(then):
            for s in range(S):
                @pl.when(zh != c * S + s)
                def _():
                    remote(ps3.at[c, s], zr.at[0], zrsnd.at[c, s], zrrcv.at[0], {"zh": c * S + s}).wait_send()

                @pl.when(zh == c * S + s)
                def _():
                    total = ps3[c, s].astype(F32)
                    for k in range(3):
                        remote(ps3.at[c, s], zr.at[k], zrsnd.at[c, s], zrrcv.at[k], to("zh", 1)).wait_recv()
                        total = total + zr[k].astype(F32)
                    then(total)

        def z_first():
            z_send(acts)

        def to_latent():
            preact = full[c].astype(F32) + enc_bias[...]
            gating = jax.nn.sigmoid((preact - threshold[...]) * (1.0 / JUMP))
            value = preact * gating
            lat[c] = value.astype(BF)
            slope[c] = gating + value * (1.0 - gating) * (1.0 / JUMP)

        def to_preact_grad():
            for copy in grads_out(c):
                copy.start()
            lat[c] = (full[c].astype(F32) * slope[c]).astype(BF)

        def to_error():
            def then(total):
                row = lax.broadcasted_iota(jnp.int32, (ROWS, 1), 0)
                first = ((y * N + zh) * N + x) * ROWS
                keeps = jnp.zeros((ROWS, 1), jnp.int32)
                for i in range(ROWS):
                    keeps = jnp.where(row == i, mask[first + i], keeps)
                value = keeps.astype(F32) * (total + dec_bias[...] - acts[...].astype(F32))
                err[...] = value
                errh[...] = value.astype(BF)
                mean = jnp.sum(value * value, axis=1, keepdims=True) * (1.0 / depth)
                lane = lax.broadcasted_iota(jnp.int32, (ROWS, ROWS), 1)
                sq[...] = jnp.sum(jnp.where(row == lane, mean, 0.0), axis=0, keepdims=True)
                pltpu.make_async_copy(sq, sq_out, osem.at[C]).start()

            owned(then)
            z_send(errh)

        def to_input_grad():
            def then(total):
                ig[...] = (total - err[...]).astype(BF)

            wait_outs(c)
            owned(then)

        def dot(a, b):
            return jnp.dot(a, b, preferred_element_type=F32)

        def tokens():
            return ag[c].reshape(M, depth)

        def encode(lhs, where):
            return dot(lhs(), enc[:, where])

        def decode_back(lhs, where):
            return dot(lhs(), dec_t[:, where])

        def tiles(h):
            begin = 0
            while begin < half:
                length = min(512, half - begin)
                yield pl.ds(h * half + begin, length), length
                begin += length

        def decode(h):
            for where, length in tiles(h):
                value = dot(lat[c], dec[:, where])
                ps[c, :, :, :, where] = value.reshape(N, N, R, length).astype(BF)

        def encode_back(h):
            for where, length in tiles(h):
                value = dot(lat[c], enc_t[:, where])
                ps[c, :, :, :, where] = value.reshape(N, N, R, length).astype(BF)

        def joined(*parts):
            def run():
                for part in parts:
                    part()

            return run

        g1, l1, s1 = gather_stages(acts), layer_stages(0, tokens, encode), scatter_stages(decode)
        g2, l2, s2 = gather_stages(errh), layer_stages(1, tokens, decode_back), scatter_stages(encode_back)
        return [
            z_first,
            *g1[:-1],
            joined(g1[-1], l1[0]),
            *l1[1:-1],
            joined(l1[-1], to_latent, s1[0]),
            *s1[1:],
            to_error,
            *g2[:-1],
            joined(g2[-1], l2[0]),
            *l2[1:-1],
            joined(l2[-1], to_preact_grad, s2[0]),
            *s2[1:],
            to_input_grad,
        ]

    def turned(copies, src, dst):
        for copy in copies:
            copy.wait()

        def one(j, carry):
            where = pl.ds(pl.multiple_of(j * 256, 256), 256)
            dst[:, where] = src[where, :].T
            return carry

        lax.fori_loop(0, src.shape[0] // 256, one, 0)

    weights = [
        functools.partial(turned, [enc_copy], enc, enc_t),
        functools.partial(turned, [dec_copy, *small], dec, dec_t),
    ]
    plans = [iter(chunk(c)) for c in range(C)] + [iter(weights)]
    for c in TURNS:
        next(plans[c])()
    assert all(next(plan, None) is None for plan in plans)
    ig_copy = pltpu.make_async_copy(ig, ig_out, osem.at[C])
    ig_copy.start()
    ig_copy.wait()


def finish(sq_hbm, ig_hbm, lg_hbm, sq_out, ig_out, lg_out, sq, ig, raw, wide, isem, osem):
    parts = isem.shape[0] - 2
    length = raw.shape[0] // parts

    def rows(p):
        return pl.ds(p * length, length)

    ins = [pltpu.make_async_copy(lg_hbm.at[rows(p)], raw.at[rows(p)], isem.at[p]) for p in range(parts)]
    ins += [pltpu.make_async_copy(src, dst, isem.at[parts + n]) for n, (src, dst) in enumerate(((sq_hbm, sq), (ig_hbm, ig)))]
    outs = [pltpu.make_async_copy(wide.at[rows(p)], lg_out.at[rows(p)], osem.at[p]) for p in range(parts)]
    outs += [pltpu.make_async_copy(src, dst, osem.at[parts + n]) for n, (src, dst) in enumerate(((sq, sq_out), (ig, ig_out)))]
    for copy in ins:
        copy.start()
    for p in range(parts):
        ins[p].wait()
        wide[rows(p)] = raw[rows(p)].astype(F32)
        outs[p].start()
    for n in (parts, parts + 1):
        ins[n].wait()
        outs[n].start()
    for copy in outs:
        copy.wait()


def shards(activations, enc_weight, dec_weight, enc_bias, threshold, dec_bias, token_mask):
    depth, feats = enc_weight.shape[1:]
    half = depth // 2
    hbm = pl.BlockSpec(memory_space=pltpu.HBM)
    dma = pltpu.SemaphoreType.DMA
    scratch = [
        pltpu.VMEM((ROWS, depth), BF),
        *[pltpu.VMEM((1, feats), F32)] * 2,
        pltpu.VMEM((1, depth), F32),
        pltpu.SMEM(token_mask.shape, jnp.int32),
        pltpu.VMEM((depth, feats), BF),
        pltpu.VMEM((feats, depth), BF),
        pltpu.VMEM((feats, depth), BF),
        pltpu.VMEM((depth, feats), BF),
        pltpu.VMEM((C, N, N, R, depth), BF),
        pltpu.VMEM((C, S, ROWS, depth), BF),
        pltpu.VMEM((C, N, N, R, depth), BF),
        pltpu.VMEM((C, 2, 3, N, R, half), BF),
        pltpu.VMEM((C, 2, N, R, half), BF),
        pltpu.VMEM((C, 2, 3, R, half), BF),
        pltpu.VMEM((C, S, ROWS, depth), BF),
        pltpu.VMEM((N - 1, ROWS, depth), BF),
        pltpu.VMEM((C, HM, feats), F32),
        *[pltpu.VMEM((C, HM, feats), BF)] * 3,
        pltpu.VMEM((2, C, HM, feats), BF),
        pltpu.VMEM((C, M, feats), BF),
        pltpu.VMEM((C, M, feats), BF),
        pltpu.VMEM((C, M, feats), F32),
        pltpu.VMEM((ROWS, depth), F32),
        pltpu.VMEM((ROWS, depth), BF),
        pltpu.VMEM((1, ROWS), F32),
        pltpu.VMEM((ROWS, depth), BF),
        dma((7,)),
        dma((C + 1,)),
        dma((3,)), dma((C, S)),
        dma((C, 2)),
        dma((C, 2, 1)), dma((C, 2, 3)), dma((C, 2, 3)), dma((C, 2, 1)),
        dma((C, S)), dma((3,)),
        dma((C, PIECES)), dma((C, 4, PIECES)),
    ]
    sq, ig, lg = pl.pallas_call(
        kernel,
        out_shape=(
            jax.ShapeDtypeStruct((1, ROWS), F32),
            jax.ShapeDtypeStruct((ROWS, depth), BF),
            jax.ShapeDtypeStruct((N * N * N * ROWS, feats), BF),
        ),
        in_specs=[hbm] * 7,
        out_specs=(hbm,) * 3,
        scratch_shapes=scratch,
        compiler_params=pltpu.CompilerParams(
            collective_id=0, has_side_effects=True, vmem_limit_bytes=67043328
        ),
    )(
        activations[:, 0], enc_weight[0], dec_weight[0], enc_bias[None], threshold[None], dec_bias, token_mask,
    )
    tokens, parts = N * N * N * ROWS, 4
    sq, ig, lg = pl.pallas_call(
        finish,
        out_shape=(
            jax.ShapeDtypeStruct((1, ROWS), F32),
            jax.ShapeDtypeStruct((ROWS, depth), BF),
            jax.ShapeDtypeStruct((tokens, feats), F32),
        ),
        in_specs=[hbm] * 3,
        out_specs=(hbm,) * 3,
        scratch_shapes=[
            pltpu.VMEM((1, ROWS), F32),
            pltpu.VMEM((ROWS, depth), BF),
            pltpu.VMEM((tokens, feats), BF),
            pltpu.VMEM((tokens, feats), F32),
            dma((parts + 2,)), dma((parts + 2,)),
        ],
        compiler_params=pltpu.CompilerParams(vmem_limit_bytes=67043328),
    )(sq, ig, lg)
    return sq.reshape(ROWS, 1), lg, ig[:, None]


def solution(mesh):
    finer = Mesh(mesh.devices.reshape(2, 2, N, N, N), LAYER + FEAT)
    return jax.shard_map(
        shards,
        mesh=finer,
        in_specs=(
            P(FEAT, LAYER, None),
            P(LAYER, None, FEAT),
            P(LAYER, FEAT, None),
            P(FEAT),
            P(FEAT),
            P(LAYER, None),
            P(),
        ),
        out_specs=(P(FEAT, LAYER), P(None, FEAT), P(FEAT, LAYER, None)),
        check_vma=False,
    )
```
